16 devices in a mesh: dp: 2 (over y, z), ep: 8 (over x, core).
Axes of the slice: x: 4, y: 2, z: 1, core: 2. Of those that a mesh axis runs over, the one named last changes fastest.
The devices are a block of a 4x4x8 slice.
Arguments:
- x: bfloat16 [2, 8, 256, 4096], P('dp', 'ep'), parts along dimension 0
- expert: int32 [2, 8, 256, 8], P('dp', 'ep'), parts along dimension 0
- slot: int32 [2, 8, 256, 8], P('dp', 'ep'), parts along dimension 0
- gate: float32 [2, 8, 256, 8], P('dp', 'ep'), parts along dimension 0
- w_gate: bfloat16 [64, 4096, 1536], P('ep')
- w_up: bfloat16 [64, 4096, 1536], P('ep')
- w_down: bfloat16 [64, 1536, 4096], P('ep')
Outputs:
- y: bfloat16 [2, 8, 256, 4096], P('dp', 'ep'), parts along dimension 0
There are 2 independent parts. The reference program is written for one: setup_inputs(seed, part) draws one part's arguments, and reference() takes and returns one part's arrays. A program takes and returns all parts, laid end to end along the dimension named above; an argument that names none is the same for every part.
All inputs are finite; a program needn't handle non-finite values.
Results may differ from the reference program's by a relative error of at most 0.009.
Values are sent between devices in bfloat16 or wider.
A program may use at most 768 MiB of HBM per device.

```python
import jax
import jax.numpy as jnp

MEMBERS = 8
TOKENS = 256
D = 4096
FF = 1536
TOP = 8
EXPERTS = 64
SLOTS = 5 * TOKENS * TOP // (4 * EXPERTS)


def setup_inputs(seed: int = 0, part: int = 0) -> dict:
    own, k1, k2, k3, k4, k5, k6 = jax.random.split(jax.random.key(seed), 7)
    kx, ke, kl, kg = jax.random.split(jax.random.fold_in(own, part), 4)
    devices = (1, MEMBERS)
    place = jax.random.permutation(kl, jnp.arange(EXPERTS, dtype=jnp.uint32))
    slow = ((EXPERTS + (9 * place) % EXPERTS) << ((9 * place) // EXPERTS)) // EXPERTS
    wait = (jax.random.bits(ke, (*devices, TOKENS, EXPERTS), jnp.uint32) >> 10) * slow
    expert = jnp.argsort(wait, axis=-1)[..., :TOP].astype(jnp.int32)
    chosen = jax.nn.one_hot(expert, EXPERTS, dtype=jnp.int32)
    in_line = jnp.cumsum(chosen.reshape(*devices, TOKENS * TOP, EXPERTS), axis=2) - 1
    slot = jnp.sum(in_line.reshape(chosen.shape) * chosen, axis=-1)

    def one(key, rows, columns):
        return (jax.random.normal(key, (rows, columns), jnp.float32) * rows**-0.5).astype(jnp.bfloat16)

    def weights(key, rows, columns):
        return jax.lax.map(lambda k: one(k, rows, columns), jax.random.split(key, EXPERTS))

    return {
        "x": jax.random.normal(kx, (*devices, TOKENS, D), jnp.float32).astype(jnp.bfloat16),
        "expert": expert,
        "slot": slot,
        "gate": jax.nn.softmax(jax.random.normal(kg, expert.shape, jnp.float32)),
        "w_gate": weights(k1, D, FF),
        "w_up": weights(k2, D, FF),
        "w_down": weights(k3, FF, D),
    }


def einsum(form, a, b):
    return jnp.einsum(form, a.astype(jnp.float32), b.astype(jnp.float32))


def reference(x, expert, slot, gate, w_gate, w_up, w_down):
    to_expert = jax.nn.one_hot(expert, EXPERTS, dtype=jnp.bfloat16)
    to_slot = jax.nn.one_hot(slot, SLOTS, dtype=jnp.bfloat16)
    weighted = to_expert * gate[..., None].astype(jnp.bfloat16)
    dispatch = einsum("abtke,abtkc->abtec", to_expert, to_slot).astype(jnp.bfloat16)
    combine = einsum("abtke,abtkc->abtec", weighted, to_slot).astype(jnp.bfloat16)
    z = einsum("abtec,abtd->aebcd", dispatch, x).astype(jnp.bfloat16)
    h = jax.nn.silu(einsum("aebcd,edf->aebcf", z, w_gate))
    h = (h * einsum("aebcd,edf->aebcf", z, w_up)).astype(jnp.bfloat16)
    out = einsum("aebcf,efd->aebcd", h, w_down).astype(jnp.bfloat16)
    y = einsum("abtec,aebcd->abtd", combine, out)
    return y.astype(jnp.bfloat16)
```

```python
import functools

import jax
import jax.numpy as jnp
from jax import lax
from jax.experimental import pallas as pl
from jax.experimental.pallas import tpu as pltpu
from jax.sharding import PartitionSpec as P

F32, BF16 = jnp.float32, jnp.bfloat16
MESH = pl.DeviceIdType.MESH
KC = 512
NC = 256
XS = 4
WS = 6
RR = 6
SS = 3
LAG1, LAG2, LAG3 = 1, 3, 5
OWN, SIB, RT, RTS, FAR, FARS, LF, LFS = range(8)


def dot(a, b):
    return jnp.dot(a, b, preferred_element_type=F32)


def kernel(sizes, meta, x_hbm, wg, wu, wd, y_hbm, acc, xg, wbuf, z32, zb, disp, comb, metas, ssend, srecv, fsend, frecv,
           nsend, nrecv, yst, wsem, osem, ag_s, ag_r, m_s, m_r, sib_s, sib_r, f_s, f_r, n_s, n_r, ysem):
    tokens, d, ff, experts, slots, chips = sizes
    rows = experts * slots
    group = 2 * chips
    half = tokens // 2
    nk, nn = d // KC, d // NC
    nb_ff = ff // NC
    me = lax.axis_index("ep")
    chip, core = me // 2, me % 2

    def peer(rel):
        return {"ep": ((chip + rel // 2) % chips) * 2 + (core + rel % 2) % 2}

    def back(rel):
        return ((chips - rel // 2) % chips) * 2 + rel % 2

    first_down = nk * experts * 2

    def gate_up_copy(k, u, i):
        e, m = u // 2, u % 2
        b = i % WS
        w = (wg, wu)[m]
        return pltpu.make_async_copy(w.at[e, pl.ds(k * KC, KC), :], wbuf.at[b], wsem.at[b])

    def down_start(n, q, i):
        b = i % WS
        for p in range(2):
            for kb in range(nb_ff):
                pltpu.make_async_copy(
                    wd.at[2 * q + p, pl.ds(kb * NC, NC), pl.ds(n * NC, NC)],
                    wbuf.at[b, pl.ds(p * NC, NC), pl.ds(kb * NC, NC)],
                    wsem.at[b],
                ).start()

    def weights_wait(i):
        b = i % WS
        pltpu.make_async_copy(wbuf.at[b], wbuf.at[b], wsem.at[b]).wait()

    def block(k, rel, lo=0, n=tokens):
        return xg.at[pl.ds((k % XS) * (group * tokens) + rel * tokens + lo, n)]

    def own_copy(k):
        return pltpu.make_async_copy(x_hbm.at[:, pl.ds(k * KC, KC)], block(k, OWN), osem.at[k % XS])

    KINDS = [
        (OWN, LF, RT, 0, half),
        (OWN, RT, LF, half, half),
        (OWN, LF, RT, half, half),
        (OWN, RT, LF, 0, half),
        (OWN, SIB, SIB, 0, tokens),
        (LF, LFS, SIB, 0, tokens),
        (RT, RTS, SIB, 0, tokens),
        (LF, FAR, RT, 0, half),
        (RT, FAR, LF, half, half),
        (FAR, FARS, SIB, 0, half),
        (FAR, FARS, SIB, half, half),
    ]

    def ag(t, k):
        src, dst, to, lo, n = KINDS[t]
        s = k % XS
        return pltpu.make_async_remote_copy(
            src_ref=block(k, src, lo, n), dst_ref=block(k, dst, lo, n), send_sem=ag_s.at[t, s], recv_sem=ag_r.at[t, s],
            device_id=peer(to), device_id_type=MESH)

    def near_start(k):
        for t in (0, 1, 2, 3, 4):
            ag(t, k).start()

    def forward(k):
        for t, f in ((0, 7), (1, 8)):
            ag(t, k).wait_recv()
            ag(f, k).start()
        for t, f in ((2, 5), (3, 6)):
            ag(t, k).wait_recv()
            ag(f, k).start()

    def far_forward(k):
        for t, f in ((7, 9), (8, 10)):
            ag(t, k).wait_recv()
            ag(f, k).start()

    def sends_wait(k):
        for t in range(len(KINDS)):
            ag(t, k).wait_send()

    def meta_copy(rel):
        return pltpu.make_async_remote_copy(
            src_ref=meta, dst_ref=metas.at[back(rel)], send_sem=m_s.at[rel], recv_sem=m_r.at[back(rel)],
            device_id=peer(rel), device_id_type=MESH)

    for k in range(3):
        own_copy(k).start()
    for i in range(WS - 1):
        gate_up_copy(0, i, i).start()
    barrier = pltpu.get_barrier_semaphore()
    for rel in range(1, group):
        pl.semaphore_signal(barrier, inc=1, device_id=peer(rel), device_id_type=MESH)
    pl.semaphore_wait(barrier, group - 1)
    for rel in range(1, group):
        meta_copy(rel).start()
    own_copy(0).wait()
    near_start(0)
    metas[OWN] = meta[...]

    def zero(i, _):
        for e in range(experts):
            acc[e, i] = jnp.zeros(acc.shape[2:], F32)
        return 0

    lax.fori_loop(0, 2 * nb_ff, zero, 0)
    for rel in range(1, group):
        meta_copy(back(rel)).wait_recv()
    row_id = (lax.broadcasted_iota(jnp.int32, (rows, tokens), 0) + me * rows).astype(F32)

    def build_disp(r, _):
        m = metas[r]
        hit = jnp.zeros((rows, tokens), F32)
        for j in range(m.shape[0] // 2):
            hit = jnp.where(row_id == m[j:j + 1, :], 1.0, hit)
        disp[r] = hit.astype(BF16)
        return 0

    def build_comb(r, _):
        m = metas[r]
        top = m.shape[0] // 2
        g = jnp.zeros((rows, tokens), F32)
        for j in range(top):
            g = jnp.where(row_id == m[j:j + 1, :], m[top + j:top + j + 1, :], g)
        comb[r] = g.T.astype(BF16)
        return 0

    lax.fori_loop(0, group, build_disp, 0)
    forward(0)
    own_copy(1).wait()
    near_start(1)
    lax.fori_loop(0, group, build_comb, 0)
    far_forward(0)
    own_copy(2).wait()
    near_start(2)
    for rel in range(1, group):
        meta_copy(rel).wait_send()

    def gather(k):
        for t in (4, 5, 6, 9, 10):
            ag(t, k).wait_recv()
        for r in range(group):
            z = dot(disp[r], block(k, r)[...])
            for e in range(experts):
                z32[e, r * slots:(r + 1) * slots, :] = z[e * slots:(e + 1) * slots]

    def step(k, u, last):
        e, m = u // 2, u % 2
        i = k * (2 * experts) + u
        ahead = u + WS - 1
        if ahead < 2 * experts:
            gate_up_copy(k, ahead, i + WS - 1).start()
        elif not last:
            gate_up_copy(k + 1, ahead - 2 * experts, i + WS - 1).start()
        else:
            down_start((ahead - 2 * experts) // (experts // 2), (ahead - 2 * experts) % (experts // 2), i + WS - 1)
        weights_wait(i)
        b = i % WS
        if m == 0:
            zb[e % 2] = z32[e].astype(BF16)
        for nb in range(nb_ff):
            out = acc[e, m * nb_ff + nb] + dot(zb[e % 2], wbuf[b, :, nb * NC:(nb + 1) * NC])
            if last and m == 1:
                h = (jax.nn.silu(acc[e, nb]) * out).astype(BF16)
                at = (nb % 2) * NC
                xg[(e * (nb_ff // 2) + nb // 2) * (group * slots):(e * (nb_ff // 2) + nb // 2 + 1) * (group * slots),
                   at:at + NC] = h
            else:
                acc[e, m * nb_ff + nb] = out

    def chunk(k, _):
        @pl.when(k + 3 < nk)
        def _():
            own_copy(k + 3).start()

        gather(k)
        for u in range(2 * experts):
            step(k, u, False)
            if u == 3:
                sends_wait(k)
                forward(k + 1)

                @pl.when(k + 3 < nk)
                def _():
                    own_copy(k + 3).wait()
                    near_start(k + 3)
            if u == 11:
                far_forward(k + 1)
        return 0

    lax.fori_loop(0, nk - 1, chunk, 0)
    gather(nk - 1)
    sends_wait(nk - 1)
    for u in range(2 * experts):
        step(nk - 1, u, True)

    def sib_copy(m):
        return pltpu.make_async_remote_copy(
            src_ref=ssend.at[m % 2], dst_ref=srecv.at[m % 4], send_sem=sib_s.at[m % 2], recv_sem=sib_r.at[m % 4],
            device_id=peer(SIB), device_id_type=MESH)

    def far_copy(m, way):
        return pltpu.make_async_remote_copy(
            src_ref=fsend.at[m % SS, way], dst_ref=frecv.at[m % RR, way], send_sem=f_s.at[way, m % SS],
            recv_sem=f_r.at[way, m % RR], device_id=peer((RT, LF)[way]), device_id_type=MESH)

    def near_copy(m, way):
        return pltpu.make_async_remote_copy(
            src_ref=nsend.at[m % SS, way], dst_ref=nrecv.at[m % RR, way], send_sem=n_s.at[way, m % SS],
            recv_sem=n_r.at[way, m % RR], device_id=peer((RT, LF)[way]), device_id_type=MESH)

    def y_copy(m):
        return pltpu.make_async_copy(yst.at[m % 2], y_hbm.at[:, pl.ds(m * NC, NC)], ysem.at[m % 2])

    pairs = experts // 2
    total_pairs = nn * pairs

    def down(n):
        for e in range(experts):
            q = e // 2
            i = first_down + n * pairs + q
            b = i % WS
            if e % 2 == 0:
                ahead = q + WS - 1

                @pl.when(n * pairs + ahead < total_pairs)
                def _():
                    down_start(n + ahead // pairs, ahead % pairs, i + WS - 1)

                weights_wait(i)
            out = None
            for kb in range(nb_ff):
                at = (e * (nb_ff // 2) + kb // 2) * (group * slots)
                t = dot(xg[at:at + group * slots, (kb % 2) * NC:(kb % 2 + 1) * NC],
                        wbuf[b, (e % 2) * NC:(e % 2 + 1) * NC, kb * NC:(kb + 1) * NC])
                out = t if out is None else out + t
            z32[e, :, :NC] = out
        for r in range(group):
            rhs = z32[:, r * slots:(r + 1) * slots, :NC].reshape(rows, NC).astype(BF16)
            p = dot(comb[r], rhs)
            if r % 2:
                ssend[n % 2, r // 2] = p.astype(BF16)
            else:
                acc[n % 8, r // 2, :tokens, :] = p
        sib_copy(n).start()

    def to_far(m):
        sib_copy(m).wait_recv()
        s = m % 8
        far = acc[s, 2, :tokens, :] + srecv[m % 4, 2].astype(F32)
        fsend[m % SS, 0] = far[:half].astype(BF16)
        fsend[m % SS, 1] = far[half:].astype(BF16)
        for way in range(2):
            far_copy(m, way).start()
        for c in (0, 1, 3):
            acc[s, c, :tokens, :] = acc[s, c, :tokens, :] + srecv[m % 4, c].astype(F32)
        sib_copy(m).wait_send()

    def to_near(m):
        s = m % 8
        far_copy(m, 0).wait_recv()
        nsend[m % SS, 0, :half] = (acc[s, 1, :half, :] + frecv[m % RR, 0].astype(F32)).astype(BF16)
        nsend[m % SS, 0, half:] = acc[s, 1, half:tokens, :].astype(BF16)
        near_copy(m, 0).start()
        far_copy(m, 1).wait_recv()
        nsend[m % SS, 1, :half] = acc[s, 3, :half, :].astype(BF16)
        nsend[m % SS, 1, half:] = (acc[s, 3, half:tokens, :] + frecv[m % RR, 1].astype(F32)).astype(BF16)
        near_copy(m, 1).start()
        for way in range(2):
            far_copy(m, way).wait_send()

    def finish(m):
        for way in range(2):
            near_copy(m, way).wait_recv()

        @pl.when(m >= 2)
        def _():
            y_copy(m - 2).wait()

        s = m % 8
        total = acc[s, 0, :tokens, :] + nrecv[m % RR, 0].astype(F32) + nrecv[m % RR, 1].astype(F32)
        yst[m % 2] = total.astype(BF16)
        y_copy(m).start()
        for way in range(2):
            near_copy(m, way).wait_send()

    def columns(n, _):
        @pl.when(n < nn)
        def _():
            down(n)

        for lag, stage in ((LAG1, to_far), (LAG2, to_near), (LAG3, finish)):
            @pl.when((n >= lag) & (n < nn + lag))
            def _(lag=lag, stage=stage):
                stage(n - lag)
        return 0

    lax.fori_loop(0, nn + LAG3, columns, 0)
    for m in (nn - 2, nn - 1):
        y_copy(m).wait()


def solution(mesh):
    def body(x, expert, slot, gate, w_gate, w_up, w_down):
        x, expert, slot, gate = (v.reshape(v.shape[2:]) for v in (x, expert, slot, gate))
        tokens, d = x.shape
        top = expert.shape[1]
        experts, _, ff = w_gate.shape
        group = mesh.shape["ep"]
        chips = group // 2
        slots = 5 * tokens * top // (4 * experts * group)
        rows, all_rows = experts * slots, group * slots
        place = jnp.where(slot < slots, expert * slots + slot, -1).astype(F32)
        meta = jnp.concatenate([place.T, gate.astype(BF16).astype(F32).T], axis=0)
        any_, vmem = pl.BlockSpec(memory_space=pl.ANY), pl.BlockSpec(memory_space=pltpu.VMEM)
        dma, half = pltpu.SemaphoreType.DMA, tokens // 2
        y = pl.pallas_call(
            functools.partial(kernel, (tokens, d, ff, experts, slots, chips)),
            out_shape=jax.ShapeDtypeStruct((tokens, d), BF16),
            in_specs=[vmem, any_, any_, any_, any_],
            out_specs=any_,
            scratch_shapes=[
                pltpu.VMEM((experts, 2 * ff // NC, all_rows, NC), F32),
                pltpu.VMEM((XS * group * tokens, KC), BF16),
                pltpu.VMEM((WS, KC, ff), BF16),
                pltpu.VMEM((experts, all_rows, KC), F32),
                pltpu.VMEM((2, all_rows, KC), BF16),
                pltpu.VMEM((group, rows, tokens), BF16),
                pltpu.VMEM((group, tokens, rows), BF16),
                pltpu.VMEM((group, 2 * top, tokens), F32),
                pltpu.VMEM((2, chips, tokens, NC), BF16),
                pltpu.VMEM((4, chips, tokens, NC), BF16),
                pltpu.VMEM((SS, 2, half, NC), BF16),
                pltpu.VMEM((RR, 2, half, NC), BF16),
                pltpu.VMEM((SS, 2, tokens, NC), BF16),
                pltpu.VMEM((RR, 2, tokens, NC), BF16),
                pltpu.VMEM((2, tokens, NC), BF16),
                dma((WS,)), dma((XS,)), dma((11, XS)), dma((11, XS)), dma((group,)), dma((group,)),
                dma((2,)), dma((4,)), dma((2, SS)), dma((2, RR)), dma((2, SS)), dma((2, RR)), dma((2,)),
            ],
            compiler_params=pltpu.CompilerParams(
                collective_id=0, has_side_effects=True, vmem_limit_bytes=67043328),
            name="moe",
        )(meta, x, w_gate, w_up, w_down)
        return y.reshape(1, 1, tokens, d)

    tok = P("dp", "ep", None, None)
    w = P("ep", None, None)
    return jax.shard_map(body, mesh=mesh, in_specs=(tok, tok, tok, tok, w, w, w), out_specs=tok, check_vma=False)
```

```python
import functools

import jax
import jax.numpy as jnp
from jax import lax
from jax.experimental import pallas as pl
from jax.experimental.pallas import tpu as pltpu
from jax.sharding import PartitionSpec as P

F32, BF16 = jnp.float32, jnp.bfloat16
MESH = pl.DeviceIdType.MESH
KC = 512
NC = 256
XS = 4
WS = 6
RR = 6
SS = 4
LAG1, LAG2, LAG3 = 1, 2, 5
OWN, SIB, RT, RTS, FAR, FARS, LF, LFS = range(8)


def dot(a, b):
    return jnp.dot(a, b, preferred_element_type=F32)


def kernel(sizes, expert, slot, gate, x_hbm, wg, wu, wd, y_hbm, acc, xg, wbuf, z32, zb, disp, comb, places, gates, ssend, srecv, fsend, frecv,
           nsend, nrecv, yst, wsem, osem, ag_s, ag_r, m_s, m_r, sib_s, sib_r, f_s, f_r, n_s, n_r, ysem):
    tokens, d, ff, experts, slots, chips = sizes
    rows = experts * slots
    group = 2 * chips
    half = tokens // 2
    nk, nn = d // KC, d // NC
    nb_ff = ff // NC
    me = lax.axis_index("ep")
    chip, core = me // 2, me % 2

    def peer(rel):
        return {"ep": ((chip + rel // 2) % chips) * 2 + (core + rel % 2) % 2}

    def back(rel):
        return ((chips - rel // 2) % chips) * 2 + rel % 2

    first_down = nk * experts * 2

    def gate_up_copy(k, u, i):
        e, m = u // 2, u % 2
        b = i % WS
        w = (wg, wu)[m]
        return pltpu.make_async_copy(w.at[e, pl.ds(k * KC, KC), :], wbuf.at[b], wsem.at[b])

    def down_start(n, q, i):
        b = i % WS
        for p in range(2):
            for kb in range(nb_ff):
                pltpu.make_async_copy(
                    wd.at[2 * q + p, pl.ds(kb * NC, NC), pl.ds(n * NC, NC)],
                    wbuf.at[b, pl.ds(p * NC, NC), pl.ds(kb * NC, NC)],
                    wsem.at[b],
                ).start()

    def weights_wait(i):
        b = i % WS
        pltpu.make_async_copy(wbuf.at[b], wbuf.at[b], wsem.at[b]).wait()

    def block(k, rel, lo=0, n=tokens):
        return xg.at[pl.ds((k % XS) * (group * tokens) + rel * tokens + lo, n)]

    def own_copy(k):
        return pltpu.make_async_copy(x_hbm.at[:, pl.ds(k * KC, KC)], block(k, OWN), osem.at[k % XS])

    KINDS = [
        (OWN, LF, RT, 0, half),
        (OWN, RT, LF, half, half),
        (OWN, LF, RT, half, half),
        (OWN, RT, LF, 0, half),
        (OWN, SIB, SIB, 0, tokens),
        (LF, LFS, SIB, 0, tokens),
        (RT, RTS, SIB, 0, tokens),
        (LF, FAR, RT, 0, half),
        (RT, FAR, LF, half, half),
        (FAR, FARS, SIB, 0, half),
        (FAR, FARS, SIB, half, half),
    ]

    def ag(t, k):
        src, dst, to, lo, n = KINDS[t]
        s = k % XS
        return pltpu.make_async_remote_copy(
            src_ref=block(k, src, lo, n), dst_ref=block(k, dst, lo, n), send_sem=ag_s.at[t, s], recv_sem=ag_r.at[t, s],
            device_id=peer(to), device_id_type=MESH)

    def near_start(k):
        for t in (0, 1, 2, 3, 4):
            ag(t, k).start()

    def forward(k):
        for t, f in ((0, 7), (1, 8)):
            ag(t, k).wait_recv()
            ag(f, k).start()

    def share(k):
        for t, f in ((2, 5), (3, 6)):
            ag(t, k).wait_recv()
            ag(f, k).start()

    def far_forward(k):
        for t, f in ((7, 9), (8, 10)):
            ag(t, k).wait_recv()
            ag(f, k).start()

    def sends_wait(k):
        for t in range(len(KINDS)):
            ag(t, k).wait_send()

    def place_copy(rel):
        return pltpu.make_async_remote_copy(
            src_ref=places.at[OWN], dst_ref=places.at[back(rel)], send_sem=m_s.at[0, rel], recv_sem=m_r.at[0, back(rel)],
            device_id=peer(rel), device_id_type=MESH)

    def gate_copy(rel):
        return pltpu.make_async_remote_copy(
            src_ref=gates.at[OWN], dst_ref=gates.at[back(rel)], send_sem=m_s.at[1, rel], recv_sem=m_r.at[1, back(rel)],
            device_id=peer(rel), device_id_type=MESH)

    for k in range(2):
        own_copy(k).start()
    for i in range(WS - 2):
        gate_up_copy(0, i, i).start()
    barrier = pltpu.get_barrier_semaphore()
    for rel in range(1, group):
        pl.semaphore_signal(barrier, inc=1, device_id=peer(rel), device_id_type=MESH)
    places[OWN] = jnp.where(slot[...] < slots, expert[...] * slots + slot[...], -1).astype(F32)
    gates[OWN] = gate[...].astype(BF16).astype(F32)
    own_copy(0).wait()
    pl.semaphore_wait(barrier, group - 1)
    for t in (0, 1):
        ag(t, 0).start()
    for rel in range(1, group):
        place_copy(rel).start()
    for t in (2, 3, 4):
        ag(t, 0).start()

    def zero(i, _):
        for e in range(experts):
            acc[e, i] = jnp.zeros(acc.shape[2:], F32)
        return 0

    lax.fori_loop(0, 2 * nb_ff, zero, 0)
    forward(0)
    own_copy(1).wait()
    near_start(1)
    for rel in range(1, group):
        gate_copy(rel).start()
    for rel in range(1, group):
        place_copy(back(rel)).wait_recv()
    row_id = (lax.broadcasted_iota(jnp.int32, (rows, tokens), 0) + me * rows).astype(F32)

    def build_disp(r, _):
        m = places[r]
        hit = jnp.zeros((rows, tokens), F32)
        for j in range(m.shape[0]):
            hit = jnp.where(row_id == m[j:j + 1, :], 1.0, hit)
        disp[r] = hit.astype(BF16)
        return 0

    def build_comb(r):
        m, w = places[r], gates[r]
        row = (lax.broadcasted_iota(jnp.int32, (rows, tokens), 0) + me * rows).astype(F32)
        g = jnp.zeros((rows, tokens), F32)
        for j in range(m.shape[0]):
            g = jnp.where(row == m[j:j + 1, :], w[j:j + 1, :], g)
        comb[r] = g.T.astype(BF16)

    lax.fori_loop(0, group, build_disp, 0)
    share(0)
    far_forward(0)
    for rel in range(1, group):
        place_copy(rel).wait_send()

    def gather(k):
        for t in (4, 5, 6, 9, 10):
            ag(t, k).wait_recv()
        for r in range(group):
            z = dot(disp[r], block(k, r)[...])
            for e in range(experts):
                z32[e, r * slots:(r + 1) * slots, :] = z[e * slots:(e + 1) * slots]

    def step(k, u, last):
        e, m = u // 2, u % 2
        i = k * (2 * experts) + u
        if m == 0:
            for v in range(2):
                ahead = u + v + WS - 2
                if ahead < 2 * experts:
                    gate_up_copy(k, ahead, i + v + WS - 2).start()
                elif not last:
                    gate_up_copy(k + 1, ahead - 2 * experts, i + v + WS - 2).start()
                else:
                    q = ahead - 2 * experts
                    down_start(q // (experts // 2), q % (experts // 2), i + v + WS - 2)
            weights_wait(i)
            weights_wait(i + 1)
        b = i % WS
        if m == 0:
            zb[e % 2] = z32[e].astype(BF16)
        for nb in range(nb_ff):
            out = acc[e, m * nb_ff + nb] + dot(zb[e % 2], wbuf[b, :, nb * NC:(nb + 1) * NC])
            if last and m == 1:
                h = (jax.nn.silu(acc[e, nb]) * out).astype(BF16)
                at = (nb % 2) * NC
                xg[(e * (nb_ff // 2) + nb // 2) * (group * slots):(e * (nb_ff // 2) + nb // 2 + 1) * (group * slots),
                   at:at + NC] = h
            else:
                acc[e, m * nb_ff + nb] = out

    def chunk(k, _):
        @pl.when(k + 2 < nk)
        def _():
            own_copy(k + 2).start()

        gather(k)
        for u in range(2 * experts):
            step(k, u, False)
            if u == 3:
                sends_wait(k)
                forward(k + 1)

                @pl.when(k + 2 < nk)
                def _():
                    own_copy(k + 2).wait()
                    near_start(k + 2)

            if u == 7:
                share(k + 1)

                @pl.when(k == 0)
                def _():
                    for rel in range(1, group):
                        gate_copy(back(rel)).wait_recv()
                        gate_copy(rel).wait_send()

                build_comb(k)
            if u == 13:
                far_forward(k + 1)
        return 0

    lax.fori_loop(0, nk - 1, chunk, 0)
    gather(nk - 1)
    sends_wait(nk - 1)
    for r in range(nk - 1, group):
        build_comb(r)
    for u in range(2 * experts):
        step(nk - 1, u, True)

    def sib_copy(m):
        return pltpu.make_async_remote_copy(
            src_ref=ssend.at[m % 2], dst_ref=srecv.at[m % 4], send_sem=sib_s.at[m % 2], recv_sem=sib_r.at[m % 4],
            device_id=peer(SIB), device_id_type=MESH)

    def far_copy(m, way):
        return pltpu.make_async_remote_copy(
            src_ref=fsend.at[m % SS, way], dst_ref=frecv.at[m % RR, way], send_sem=f_s.at[way, m % SS],
            recv_sem=f_r.at[way, m % RR], device_id=peer((RT, LF)[way]), device_id_type=MESH)

    def near_copy(m, way):
        return pltpu.make_async_remote_copy(
            src_ref=nsend.at[m % SS, way], dst_ref=nrecv.at[m % RR, way], send_sem=n_s.at[way, m % SS],
            recv_sem=n_r.at[way, m % RR], device_id=peer((RT, LF)[way]), device_id_type=MESH)

    def y_copy(m):
        return pltpu.make_async_copy(yst.at[m % 2], y_hbm.at[:, pl.ds(m * NC, NC)], ysem.at[m % 2])

    pairs = experts // 2
    total_pairs = nn * pairs

    def down(n, first, last):
        for e in range(first, last):
            q = e // 2
            i = first_down + n * pairs + q
            b = i % WS
            if e % 2 == 0:
                ahead = q + WS - 2

                @pl.when(n * pairs + ahead < total_pairs)
                def _():
                    down_start(n + ahead // pairs, ahead % pairs, i + WS - 2)

                weights_wait(i)
            out = None
            for kb in range(nb_ff):
                at = (e * (nb_ff // 2) + kb // 2) * (group * slots)
                t = dot(xg[at:at + group * slots, (kb % 2) * NC:(kb % 2 + 1) * NC],
                        wbuf[b, (e % 2) * NC:(e % 2 + 1) * NC, kb * NC:(kb + 1) * NC])
                out = t if out is None else out + t
            z32[e, :, :NC] = out

    def combine(n):
        for r in range(group):
            rhs = z32[:, r * slots:(r + 1) * slots, :NC].reshape(rows, NC).astype(BF16)
            p = dot(comb[r], rhs)
            if r % 2:
                ssend[n % 2, r // 2] = p.astype(BF16)
            else:
                acc[n % 8, r // 2, :tokens, :] = p
        sib_copy(n).start()

    def to_far(m):
        sib_copy(m).wait_recv()
        s = m % 8
        far = acc[s, 2, :tokens, :] + srecv[m % 4, 2].astype(F32)
        fsend[m % SS, 0] = far[:half].astype(BF16)
        fsend[m % SS, 1] = far[half:].astype(BF16)
        for way in range(2):
            far_copy(m, way).start()
        for c in (0, 1, 3):
            acc[s, c, :tokens, :] = acc[s, c, :tokens, :] + srecv[m % 4, c].astype(F32)
        sib_copy(m).wait_send()

    def to_near(m):
        s = m % 8
        far_copy(m, 0).wait_recv()
        nsend[m % SS, 0, :half] = (acc[s, 1, :half, :] + frecv[m % RR, 0].astype(F32)).astype(BF16)
        nsend[m % SS, 0, half:] = acc[s, 1, half:tokens, :].astype(BF16)
        near_copy(m, 0).start()
        far_copy(m, 1).wait_recv()
        nsend[m % SS, 1, :half] = acc[s, 3, :half, :].astype(BF16)
        nsend[m % SS, 1, half:] = (acc[s, 3, half:tokens, :] + frecv[m % RR, 1].astype(F32)).astype(BF16)
        near_copy(m, 1).start()
        for way in range(2):
            far_copy(m, way).wait_send()

    def finish(m):
        for way in range(2):
            near_copy(m, way).wait_recv()

        @pl.when(m >= 2)
        def _():
            y_copy(m - 2).wait()

        s = m % 8
        total = acc[s, 0, :tokens, :] + nrecv[m % RR, 0].astype(F32) + nrecv[m % RR, 1].astype(F32)
        yst[m % 2] = total.astype(BF16)
        y_copy(m).start()
        for way in range(2):
            near_copy(m, way).wait_send()

    def columns(n, _):
        @pl.when(n < nn)
        def _():
            down(n, 0, experts // 2)

        for lag, stage in ((LAG1, to_far), (LAG2, to_near), (LAG3, finish)):
            @pl.when((n >= lag) & (n < nn + lag))
            def _(lag=lag, stage=stage):
                stage(n - lag)

        @pl.when(n < nn)
        def _():
            down(n, experts // 2, experts)
            combine(n)
        return 0

    lax.fori_loop(0, nn + LAG3, columns, 0)
    for m in (nn - 2, nn - 1):
        y_copy(m).wait()


def solution(mesh):
    def body(x, expert, slot, gate, w_gate, w_up, w_down):
        x, expert, slot, gate = (v.reshape(v.shape[2:]) for v in (x, expert, slot, gate))
        tokens, d = x.shape
        top = expert.shape[1]
        experts, _, ff = w_gate.shape
        group = mesh.shape["ep"]
        chips = group // 2
        slots = 5 * tokens * top // (4 * experts * group)
        rows, all_rows = experts * slots, group * slots
        any_, vmem = pl.BlockSpec(memory_space=pl.ANY), pl.BlockSpec(memory_space=pltpu.VMEM)
        dma, half = pltpu.SemaphoreType.DMA, tokens // 2
        y = pl.pallas_call(
            functools.partial(kernel, (tokens, d, ff, experts, slots, chips)),
            out_shape=jax.ShapeDtypeStruct((tokens, d), BF16),
            in_specs=[vmem, vmem, vmem, any_, any_, any_, any_],
            out_specs=any_,
            scratch_shapes=[
                pltpu.VMEM((experts, 2 * ff // NC, all_rows, NC), F32),
                pltpu.VMEM((XS * group * tokens, KC), BF16),
                pltpu.VMEM((WS, KC, ff), BF16),
                pltpu.VMEM((experts, all_rows, KC), F32),
                pltpu.VMEM((2, all_rows, KC), BF16),
                pltpu.VMEM((group, rows, tokens), BF16),
                pltpu.VMEM((group, tokens, rows), BF16),
                pltpu.VMEM((group, top, tokens), F32),
                pltpu.VMEM((group, top, tokens), F32),
                pltpu.VMEM((2, chips, tokens, NC), BF16),
                pltpu.VMEM((4, chips, tokens, NC), BF16),
                pltpu.VMEM((SS, 2, half, NC), BF16),
                pltpu.VMEM((RR, 2, half, NC), BF16),
                pltpu.VMEM((SS, 2, tokens, NC), BF16),
                pltpu.VMEM((RR, 2, tokens, NC), BF16),
                pltpu.VMEM((2, tokens, NC), BF16),
                dma((WS,)), dma((XS,)), dma((11, XS)), dma((11, XS)), dma((2, group)), dma((2, group)),
                dma((2,)), dma((4,)), dma((2, SS)), dma((2, RR)), dma((2, SS)), dma((2, RR)), dma((2,)),
            ],
            compiler_params=pltpu.CompilerParams(
                collective_id=0, has_side_effects=True, vmem_limit_bytes=67043328),
            name="moe",
        )(expert.T, slot.T, gate.T, x, w_gate, w_up, w_down)
        return y.reshape(1, 1, tokens, d)

    tok = P("dp", "ep", None, None)
    w = P("ep", None, None)
    return jax.shard_map(body, mesh=mesh, in_specs=(tok, tok, tok, tok, w, w, w), out_specs=tok, check_vma=False)
```

```python
import functools

import jax
import jax.numpy as jnp
from jax import lax
from jax.experimental import pallas as pl
from jax.experimental.pallas import tpu as pltpu
from jax.sharding import PartitionSpec as P

F32, BF16 = jnp.float32, jnp.bfloat16
MESH = pl.DeviceIdType.MESH
KC = 512
NC = 256
XS = 4
WS = 6
RR = 6
SS = 4
LAG1, LAG2, LAG3 = 1, 2, 5
OWN, SIB, RT, RTS, FAR, FARS, LF, LFS = range(8)


def dot(a, b):
    return jnp.dot(a, b, preferred_element_type=F32)


def kernel(sizes, expert, slot, gate, x_hbm, wg, wu, wd, y_hbm, acc, xg, wbuf, z32, zb, disp, comb, places, gates, ssend, srecv, fsend, frecv,
           nsend, nrecv, yst, wsem, osem, ag_s, ag_r, m_s, m_r, sib_s, sib_r, f_s, f_r, n_s, n_r, ysem):
    tokens, d, ff, experts, slots, chips = sizes
    rows = experts * slots
    group = 2 * chips
    half = tokens // 2
    nk, nn = d // KC, d // NC
    nb_ff = ff // NC
    me = lax.axis_index("ep")
    chip, core = me // 2, me % 2

    def peer(rel):
        return {"ep": ((chip + rel // 2) % chips) * 2 + (core + rel % 2) % 2}

    def back(rel):
        return ((chips - rel // 2) % chips) * 2 + rel % 2

    first_down = nk * experts * 2

    def gate_up_copy(k, u, i):
        e, m = u // 2, u % 2
        b = i % WS
        w = (wg, wu)[m]
        return pltpu.make_async_copy(w.at[e, pl.ds(k * KC, KC), :], wbuf.at[b], wsem.at[b])

    def down_start(n, q, i):
        b = i % WS
        for p in range(2):
            for kb in range(nb_ff):
                pltpu.make_async_copy(
                    wd.at[2 * q + p, pl.ds(kb * NC, NC), pl.ds(n * NC, NC)],
                    wbuf.at[b, pl.ds(p * NC, NC), pl.ds(kb * NC, NC)],
                    wsem.at[b],
                ).start()

    def weights_wait(i):
        b = i % WS
        pltpu.make_async_copy(wbuf.at[b], wbuf.at[b], wsem.at[b]).wait()

    def block(k, rel, lo=0, n=tokens):
        return xg.at[pl.ds((k % XS) * (group * tokens) + rel * tokens + lo, n)]

    def own_copy(k):
        return pltpu.make_async_copy(x_hbm.at[:, pl.ds(k * KC, KC)], block(k, OWN), osem.at[k % XS])

    KINDS = [
        (OWN, LF, RT, 0, half),
        (OWN, RT, LF, half, half),
        (OWN, LF, RT, half, half),
        (OWN, RT, LF, 0, half),
        (OWN, SIB, SIB, 0, tokens),
        (LF, LFS, SIB, 0, tokens),
        (RT, RTS, SIB, 0, tokens),
        (LF, FAR, RT, 0, half),
        (RT, FAR, LF, half, half),
        (FAR, FARS, SIB, 0, half),
        (FAR, FARS, SIB, half, half),
    ]

    def ag(t, k):
        src, dst, to, lo, n = KINDS[t]
        s = k % XS
        return pltpu.make_async_remote_copy(
            src_ref=block(k, src, lo, n), dst_ref=block(k, dst, lo, n), send_sem=ag_s.at[t, s], recv_sem=ag_r.at[t, s],
            device_id=peer(to), device_id_type=MESH)

    def near_start(k):
        for t in (0, 1, 2, 3, 4):
            ag(t, k).start()

    def forward(k):
        for t, f in ((0, 7), (1, 8)):
            ag(t, k).wait_recv()
            ag(f, k).start()

    def share(k):
        for t, f in ((2, 5), (3, 6)):
            ag(t, k).wait_recv()
            ag(f, k).start()

    def far_forward(k):
        for t, f in ((7, 9), (8, 10)):
            ag(t, k).wait_recv()
            ag(f, k).start()

    def sends_wait(k):
        for t in range(len(KINDS)):
            ag(t, k).wait_send()

    def place_copy(rel):
        return pltpu.make_async_remote_copy(
            src_ref=places.at[OWN], dst_ref=places.at[back(rel)], send_sem=m_s.at[0, rel], recv_sem=m_r.at[0, back(rel)],
            device_id=peer(rel), device_id_type=MESH)

    def gate_copy(rel):
        return pltpu.make_async_remote_copy(
            src_ref=gates.at[OWN], dst_ref=gates.at[back(rel)], send_sem=m_s.at[1, rel], recv_sem=m_r.at[1, back(rel)],
            device_id=peer(rel), device_id_type=MESH)

    for k in range(2):
        own_copy(k).start()
    for i in range(WS - 2):
        gate_up_copy(0, i, i).start()
    barrier = pltpu.get_barrier_semaphore()
    for rel in range(1, group):
        pl.semaphore_signal(barrier, inc=1, device_id=peer(rel), device_id_type=MESH)
    places[OWN] = jnp.where(slot[...] < slots, expert[...] * slots + slot[...], -1).astype(F32)
    gates[OWN] = gate[...].astype(BF16).astype(F32)
    own_copy(0).wait()
    pl.semaphore_wait(barrier, group - 1)
    for t in (0, 1):
        ag(t, 0).start()
    for rel in range(1, group):
        place_copy(rel).start()
    for t in (2, 3, 4):
        ag(t, 0).start()

    def zero(i, _):
        for e in range(experts):
            acc[e, i] = jnp.zeros(acc.shape[2:], F32)
        return 0

    lax.fori_loop(0, 2 * nb_ff, zero, 0)
    forward(0)
    own_copy(1).wait()
    near_start(1)
    for rel in range(1, group):
        gate_copy(rel).start()
    for rel in range(1, group):
        place_copy(back(rel)).wait_recv()
    row_id = (lax.broadcasted_iota(jnp.int32, (rows, tokens), 0) + me * rows).astype(F32)

    def build_disp(r, _):
        m = places[r]
        hit = jnp.zeros((rows, tokens), F32)
        for j in range(m.shape[0]):
            hit = jnp.where(row_id == m[j:j + 1, :], 1.0, hit)
        disp[r] = hit.astype(BF16)
        return 0

    def build_comb(r):
        m, w = places[r], gates[r]
        row = (lax.broadcasted_iota(jnp.int32, (rows, tokens), 0) + me * rows).astype(F32)
        g = jnp.zeros((rows, tokens), F32)
        for j in range(m.shape[0]):
            g = jnp.where(row == m[j:j + 1, :], w[j:j + 1, :], g)
        comb[r] = g.T.astype(BF16)

    lax.fori_loop(0, group, build_disp, 0)
    share(0)
    for rel in range(1, group):
        place_copy(rel).wait_send()

    def gather_from(k, r):
        z = dot(disp[r], block(k, r)[...])
        for e in range(experts):
            z32[e, r * slots:(r + 1) * slots, :] = z[e * slots:(e + 1) * slots]

    def gather(k):
        for t in (4, 5, 6, 9, 10):
            ag(t, k).wait_recv()
        for r in range(group):
            gather_from(k, r)

    def step(k, u, last):
        e, m = u // 2, u % 2
        i = k * (2 * experts) + u
        if m == 0:
            for v in range(2):
                ahead = u + v + WS - 2
                if ahead < 2 * experts:
                    gate_up_copy(k, ahead, i + v + WS - 2).start()
                elif not last:
                    gate_up_copy(k + 1, ahead - 2 * experts, i + v + WS - 2).start()
                else:
                    q = ahead - 2 * experts
                    down_start(q // (experts // 2), q % (experts // 2), i + v + WS - 2)
            weights_wait(i)
            weights_wait(i + 1)
        b = i % WS
        if m == 0:
            zb[e % 2] = z32[e].astype(BF16)
        for nb in range(nb_ff):
            out = acc[e, m * nb_ff + nb] + dot(zb[e % 2], wbuf[b, :, nb * NC:(nb + 1) * NC])
            if last and m == 1:
                h = (jax.nn.silu(acc[e, nb]) * out).astype(BF16)
                at = (nb % 2) * NC
                xg[(e * (nb_ff // 2) + nb // 2) * (group * slots):(e * (nb_ff // 2) + nb // 2 + 1) * (group * slots),
                   at:at + NC] = h
            else:
                acc[e, m * nb_ff + nb] = out

    def chunk(k, _):
        @pl.when(k + 2 < nk)
        def _():
            own_copy(k + 2).start()

        for u in range(2 * experts):
            step(k, u, False)
            if u == 3:
                sends_wait(k)
                forward(k + 1)

                @pl.when(k + 2 < nk)
                def _():
                    own_copy(k + 2).wait()
                    near_start(k + 2)

            if u == 7:
                share(k + 1)

                @pl.when(k == 0)
                def _():
                    for rel in range(1, group):
                        gate_copy(back(rel)).wait_recv()
                        gate_copy(rel).wait_send()

                build_comb(k)
            if u == 13:
                far_forward(k + 1)
        gather(k + 1)
        return 0

    ag(4, 0).wait_recv()
    for r in (OWN, SIB, RT, LF):
        gather_from(0, r)
    far_forward(0)
    ag(5, 0).wait_recv()
    ag(6, 0).wait_recv()
    for r in (LFS, RTS, FAR):
        gather_from(0, r)
    ag(9, 0).wait_recv()
    ag(10, 0).wait_recv()
    gather_from(0, FARS)
    lax.fori_loop(0, nk - 1, chunk, 0)
    sends_wait(nk - 1)
    for r in range(nk - 1, group):
        build_comb(r)
    for u in range(2 * experts):
        step(nk - 1, u, True)

    def sib_copy(m):
        return pltpu.make_async_remote_copy(
            src_ref=ssend.at[m % 2], dst_ref=srecv.at[m % 4], send_sem=sib_s.at[m % 2], recv_sem=sib_r.at[m % 4],
            device_id=peer(SIB), device_id_type=MESH)

    def far_copy(m, way):
        return pltpu.make_async_remote_copy(
            src_ref=fsend.at[m % SS, way], dst_ref=frecv.at[m % RR, way], send_sem=f_s.at[way, m % SS],
            recv_sem=f_r.at[way, m % RR], device_id=peer((RT, LF)[way]), device_id_type=MESH)

    def near_copy(m, way):
        return pltpu.make_async_remote_copy(
            src_ref=nsend.at[m % SS, way], dst_ref=nrecv.at[m % RR, way], send_sem=n_s.at[way, m % SS],
            recv_sem=n_r.at[way, m % RR], device_id=peer((RT, LF)[way]), device_id_type=MESH)

    def y_copy(m):
        return pltpu.make_async_copy(yst.at[m % 2], y_hbm.at[:, pl.ds(m * NC, NC)], ysem.at[m % 2])

    pairs = experts // 2
    total_pairs = nn * pairs

    def down(n, first, last):
        i0 = first_down + n * pairs
        for q in range(first // 2, last // 2):
            ahead = q + WS - 2

            @pl.when(n * pairs + ahead < total_pairs)
            def _(q=q, ahead=ahead):
                down_start(n + ahead // pairs, ahead % pairs, i0 + q + WS - 2)

        for q in range(first // 2, last // 2):
            weights_wait(i0 + q)
        for e in range(first, last):
            b = (i0 + e // 2) % WS
            out = None
            for kb in range(nb_ff):
                at = (e * (nb_ff // 2) + kb // 2) * (group * slots)
                t = dot(xg[at:at + group * slots, (kb % 2) * NC:(kb % 2 + 1) * NC],
                        wbuf[b, (e % 2) * NC:(e % 2 + 1) * NC, kb * NC:(kb + 1) * NC])
                out = t if out is None else out + t
            z32[e, :, :NC] = out

    def combine(n):
        for r in range(group):
            rhs = z32[:, r * slots:(r + 1) * slots, :NC].reshape(rows, NC).astype(BF16)
            p = dot(comb[r], rhs)
            if r % 2:
                ssend[n % 2, r // 2] = p.astype(BF16)
            else:
                acc[n % 8, r // 2, :tokens, :] = p
        sib_copy(n).start()

    def to_far(m):
        sib_copy(m).wait_recv()
        s = m % 8
        far = acc[s, 2, :tokens, :] + srecv[m % 4, 2].astype(F32)
        fsend[m % SS, 0] = far[:half].astype(BF16)
        fsend[m % SS, 1] = far[half:].astype(BF16)
        for way in range(2):
            far_copy(m, way).start()
        for c in (0, 1, 3):
            acc[s, c, :tokens, :] = acc[s, c, :tokens, :] + srecv[m % 4, c].astype(F32)
        sib_copy(m).wait_send()

    def to_near(m):
        s = m % 8
        far_copy(m, 0).wait_recv()
        nsend[m % SS, 0, :half] = (acc[s, 1, :half, :] + frecv[m % RR, 0].astype(F32)).astype(BF16)
        nsend[m % SS, 0, half:] = acc[s, 1, half:tokens, :].astype(BF16)
        near_copy(m, 0).start()
        far_copy(m, 1).wait_recv()
        nsend[m % SS, 1, :half] = acc[s, 3, :half, :].astype(BF16)
        nsend[m % SS, 1, half:] = (acc[s, 3, half:tokens, :] + frecv[m % RR, 1].astype(F32)).astype(BF16)
        near_copy(m, 1).start()
        for way in range(2):
            far_copy(m, way).wait_send()

    def finish(m):
        for way in range(2):
            near_copy(m, way).wait_recv()

        @pl.when(m >= 2)
        def _():
            y_copy(m - 2).wait()

        s = m % 8
        total = acc[s, 0, :tokens, :] + nrecv[m % RR, 0].astype(F32) + nrecv[m % RR, 1].astype(F32)
        yst[m % 2] = total.astype(BF16)
        y_copy(m).start()
        for way in range(2):
            near_copy(m, way).wait_send()

    def columns(n, _):
        @pl.when(n < nn)
        def _():
            down(n, 0, experts // 2)

        for lag, stage in ((LAG1, to_far), (LAG2, to_near), (LAG3, finish)):
            @pl.when((n >= lag) & (n < nn + lag))
            def _(lag=lag, stage=stage):
                stage(n - lag)

        @pl.when(n < nn)
        def _():
            down(n, experts // 2, experts)
            combine(n)
        return 0

    lax.fori_loop(0, nn + LAG3, columns, 0)
    for m in (nn - 2, nn - 1):
        y_copy(m).wait()


def solution(mesh):
    def body(x, expert, slot, gate, w_gate, w_up, w_down):
        x, expert, slot, gate = (v.reshape(v.shape[2:]) for v in (x, expert, slot, gate))
        tokens, d = x.shape
        top = expert.shape[1]
        experts, _, ff = w_gate.shape
        group = mesh.shape["ep"]
        chips = group // 2
        slots = 5 * tokens * top // (4 * experts * group)
        rows, all_rows = experts * slots, group * slots
        any_, vmem = pl.BlockSpec(memory_space=pl.ANY), pl.BlockSpec(memory_space=pltpu.VMEM)
        dma, half = pltpu.SemaphoreType.DMA, tokens // 2
        y = pl.pallas_call(
            functools.partial(kernel, (tokens, d, ff, experts, slots, chips)),
            out_shape=jax.ShapeDtypeStruct((tokens, d), BF16),
            in_specs=[vmem, vmem, vmem, any_, any_, any_, any_],
            out_specs=any_,
            scratch_shapes=[
                pltpu.VMEM((experts, 2 * ff // NC, all_rows, NC), F32),
                pltpu.VMEM((XS * group * tokens, KC), BF16),
                pltpu.VMEM((WS, KC, ff), BF16),
                pltpu.VMEM((experts, all_rows, KC), F32),
                pltpu.VMEM((2, all_rows, KC), BF16),
                pltpu.VMEM((group, rows, tokens), BF16),
                pltpu.VMEM((group, tokens, rows), BF16),
                pltpu.VMEM((group, top, tokens), F32),
                pltpu.VMEM((group, top, tokens), F32),
                pltpu.VMEM((2, chips, tokens, NC), BF16),
                pltpu.VMEM((4, chips, tokens, NC), BF16),
                pltpu.VMEM((SS, 2, half, NC), BF16),
                pltpu.VMEM((RR, 2, half, NC), BF16),
                pltpu.VMEM((SS, 2, tokens, NC), BF16),
                pltpu.VMEM((RR, 2, tokens, NC), BF16),
                pltpu.VMEM((2, tokens, NC), BF16),
                dma((WS,)), dma((XS,)), dma((11, XS)), dma((11, XS)), dma((2, group)), dma((2, group)),
                dma((2,)), dma((4,)), dma((2, SS)), dma((2, RR)), dma((2, SS)), dma((2, RR)), dma((2,)),
            ],
            compiler_params=pltpu.CompilerParams(
                collective_id=0, has_side_effects=True, vmem_limit_bytes=67043328),
            name="moe",
        )(expert.T, slot.T, gate.T, x, w_gate, w_up, w_down)
        return y.reshape(1, 1, tokens, d)

    tok = P("dp", "ep", None, None)
    w = P("ep", None, None)
    return jax.shard_map(body, mesh=mesh, in_specs=(tok, tok, tok, tok, w, w, w), out_specs=tok, check_vma=False)
```
